512 devices in a mesh: section: 4 (over y_lo), dp: 32 (over y_hi, z, core), tensor: 4 (over x).
Axes of the slice: x: 4, y: 8 (y_hi: 2, y_lo: 4; y = y_hi * 4 + y_lo), z: 8, core: 2. Of those that a mesh axis runs over, the one named last changes fastest.
Arguments:
- cotangent: bfloat16 [2, 4096, 8192], P(None, 'dp', 'tensor'), may hold values from -6 to 6
- stash: bfloat16 [4, 2, 4096, 8192], P('section', None, 'dp', 'tensor'), may hold values from -0.0625 to 0.0625
- factor_a: bfloat16 [4, 1024, 8192], P('section', 'dp', 'tensor'), may hold values from -0.0625 to 0.0625
- factor_b: bfloat16 [4, 8192, 1024], P('section', ('tensor', 'dp')), may hold values from -0.1875 to 0.1875
- block_vals: bfloat16 [4, 128, 128, 128], P('section', ('dp', 'tensor')), may hold values from -0.25 to 0.25
- block_rows: int32 [4, 128], P('section'), may hold values from 0 to 63, as said below
- block_cols: int32 [4, 128], P('section'), may hold values from 0 to 63, as said below
Outputs:
- grad_in: bfloat16 [4, 2, 4096, 8192], P('section', None, 'dp', 'tensor')
- block_grad: float32 [4, 128, 128, 128], P('section', ('dp', 'tensor'))
The draws below stay inside these ranges and needn't reach their ends.
Inputs may be any that keep to these rules, and one draw needn't show every extreme that they name: The support lies inside the diagonal part of each tensor shard. Within a section all (block_rows, block_cols) pairs are distinct. For every dp index o < 32, tensor index t < 4 and slot k < 1, the block at position (o * 4 + t) + k has both its row and its column block index in [t * 8192 // (128 * 4), (t + 1) * 8192 // (128 * 4)). `block_cols`: drawn together with block_rows; the same promise holds.
All inputs are finite; a program needn't handle non-finite values.
Results may differ from the reference program's by a relative error of at most 0.024.
Values may be sent and summed in bfloat16 or wider, within the bound.
No kernel may reach another device: no remote copies, remote signals or barrier semaphores. Data moves between devices by JAX's collectives and lax.ppermute only.
A program may use at most 128 MiB of HBM per device.

```python
import jax
import jax.numpy as jnp
from jax import lax

D = 8192
R = 1024
BS = 128
BLK = 1
M = 2
TOK_DEV = 128
TOKENS = 4096
BLOCKS = 128
N_SECTION = 4
N_DP = 32
N_TENSOR = 4


def support_pairs(key):
    local_count = D // (BS * N_TENSOR)
    needed = N_DP * BLK
    base = jax.random.fold_in(key, 7)
    keys = jax.random.split(base, N_SECTION * N_TENSOR)
    picks = jax.vmap(lambda one_key: jax.random.permutation(one_key, local_count * local_count)[:needed])(keys)
    picks = picks.astype(jnp.int32).reshape(N_SECTION, N_TENSOR, N_DP, BLK).transpose(0, 2, 1, 3)
    offsets = jnp.arange(N_TENSOR, dtype=jnp.int32).reshape(1, 1, N_TENSOR, 1) * local_count
    row_ids = picks // local_count + offsets
    col_ids = picks % local_count + offsets
    return (row_ids.reshape(N_SECTION, -1).astype(jnp.int32), col_ids.reshape(N_SECTION, -1).astype(jnp.int32))


def draw_block_rows(key, part):
    return support_pairs(key)[0]


def draw_block_cols(key, part):
    return support_pairs(key)[1]


def level_of(stream_key, shape, cuts, low, top_value):
    def one(axis_at, shards_of):
        heights = jax.random.uniform(jax.random.fold_in(jax.random.fold_in(stream_key, 6), axis_at), (shards_of,), jnp.float32, low / len(cuts), top_value / len(cuts))
        return jnp.repeat(jnp.exp(heights), shape[axis_at] // shards_of).reshape((-1,) + (1,) * (len(shape) - axis_at - 1))

    factor_of = one(*cuts[0])
    for cut in cuts[1:]:
        factor_of = factor_of * one(*cut)
    return factor_of


def bell_draw(own_key, extent, width, bound, pieces=(), kind=jnp.bfloat16):
    factor_of = level_of(own_key, extent, pieces, -0.22, 0.18) if pieces else 1.0
    drawn = jax.random.normal(own_key, extent, jnp.float32) * width * factor_of
    return jnp.minimum(jnp.maximum(drawn, -bound), bound).astype(kind)


def setup_inputs(seed: int = 0) -> dict:
    key_of = jax.random.split(jax.random.key(seed), 8)
    return {
        "cotangent": bell_draw(key_of[0], (M, TOKENS, D), 1.0, 6.0, ((1, 32), (2, 4))),
        "stash": bell_draw(key_of[1], (N_SECTION, M, TOKENS, D), ((M * TOKENS) ** -0.5), 0.0625, ((0, 4), (2, 32), (3, 4))),
        "factor_a": bell_draw(key_of[2], (N_SECTION, R, D), D ** -0.5, 0.0625, ((0, 4), (1, 32), (2, 4))),
        "factor_b": bell_draw(key_of[3], (N_SECTION, D, R), R ** -0.5, 0.1875, ((0, 4), (1, 128))),
        "block_vals": bell_draw(key_of[4], (N_SECTION, BLOCKS, BS, BS), (0.5 * BS ** -0.5), 0.25, ((0, 4), (1, 128))),
        "block_rows": draw_block_rows(jax.random.fold_in(key_of[7], 71), 0),
        "block_cols": draw_block_cols(jax.random.fold_in(key_of[7], 71), 0),
    }


def reference(cotangent, stash, factor_a, factor_b, block_vals, block_rows, block_cols):
    block_count = D // BS
    incoming = cotangent
    grads_in = [None] * N_SECTION
    grads_blocks = [None] * N_SECTION
    for section_idx in reversed(range(N_SECTION)):
        factor_left = factor_a[section_idx]
        factor_right = factor_b[section_idx]
        values = block_vals[section_idx].astype(jnp.float32)
        row_ids = block_rows[section_idx].astype(jnp.int32)
        col_ids = block_cols[section_idx].astype(jnp.int32)
        partial_grad = jnp.zeros((N_DP, BLOCKS, BS, BS), jnp.float32)
        outputs = []
        for batch_idx in range(M):
            cot_now = incoming[batch_idx]
            rank_act = jnp.dot(cot_now, factor_left.T, preferred_element_type=jnp.float32).astype(jnp.bfloat16)
            picked_cot = jnp.take(cot_now.reshape(TOKENS, block_count, BS), col_ids, axis=1).astype(jnp.float32)
            sparse_terms = jnp.einsum("tnc,nrc->tnr", picked_cot, values)
            sparse_grad = jnp.zeros((TOKENS, block_count, BS), jnp.float32).at[:, row_ids].add(sparse_terms)
            grad_out = jnp.dot(rank_act, factor_right.T, preferred_element_type=jnp.float32) + sparse_grad.reshape(TOKENS, D)
            outputs.append(grad_out.astype(jnp.bfloat16))
            picked_in = jnp.take(stash[section_idx, batch_idx].reshape(TOKENS, block_count, BS), row_ids, axis=1).astype(jnp.float32)
            partial_grad = partial_grad + jnp.einsum(
                "ptnr,ptnc->pnrc",
                picked_in.reshape(N_DP, TOK_DEV, BLOCKS, BS),
                picked_cot.reshape(N_DP, TOK_DEV, BLOCKS, BS),
            )
        rounded = lax.optimization_barrier(partial_grad.astype(jnp.bfloat16))
        grads_blocks[section_idx] = jnp.sum(rounded.astype(jnp.float32), axis=0)
        incoming = jnp.stack(outputs)
        grads_in[section_idx] = incoming
    return jnp.stack(grads_in), jnp.stack(grads_blocks)
```

```python
import jax
import jax.numpy as jnp
from jax import lax
from jax.experimental import pallas as pl
from jax.experimental.pallas import tpu as pltpu
from jax.sharding import PartitionSpec as P

BF = jnp.bfloat16
F32 = jnp.float32
FAR = 2
CORES = 2
LIMIT = pltpu.CompilerParams(vmem_limit_bytes=20 * 1024 * 1024)


def contract_last(a, b):
    return lax.dot_general(a, b, (((1,), (1,)), ((), ())), preferred_element_type=F32)


def contract_first(a, b):
    return lax.dot_general(a, b, (((0,), (0,)), ((), ())), preferred_element_type=F32)


def block_at(pos, size):
    return pl.ds(pl.multiple_of(pos * size, size), size)


def whole(shape):
    zeros = (0,) * len(shape)
    return pl.BlockSpec(shape, lambda i: zeros)


SCALARS = pl.BlockSpec(memory_space=pltpu.SMEM)
GRID = 4


def cost(flops, size):
    return pl.CostEstimate(flops=flops, bytes_accessed=size, transcendentals=0)


def both_cores(core, mine_ref, other_ref, joined_ref):
    joined_ref[:, core] = mine_ref[...]
    joined_ref[:, 1 - core] = other_ref[...]
    _, _, _, width = joined_ref.shape
    return joined_ref[...].reshape(-1, width)


def rank_kernel(meta_ref, u_ref, mine_ref, other_ref, o_ref, joined_ref):
    weight = both_cores(meta_ref[0], mine_ref, other_ref, joined_ref)
    product = contract_last(u_ref[...], weight).astype(BF)
    for i in range(o_ref.shape[0]):
        o_ref[i] = product


def rank_partial(meta, u, mine, other, copies):
    tokens, width = u.shape
    pieces, rows, _ = mine.shape
    step = pieces // GRID
    rank = pieces * rows * CORES
    shard = pl.BlockSpec((step, rows, width), lambda i: (i, 0, 0))
    return pl.pallas_call(
        rank_kernel,
        grid=(GRID,),
        in_specs=[SCALARS, whole((tokens, width)), shard, shard],
        out_specs=pl.BlockSpec((copies, tokens, rank // GRID), lambda i: (0, 0, i)),
        out_shape=pltpu.HBM((copies, tokens, rank), BF),
        scratch_shapes=[pltpu.VMEM((step, CORES, rows, width), BF)],
        cost_estimate=cost(2 * tokens * width * rank, 2 * width * rank),
        compiler_params=LIMIT,
        name="rank_partial",
    )(meta, u, mine, other)


def sparse_kernel(meta_ref, rows_ref, cols_ref, u_ref, mine_ref, other_ref, o_ref, t_ref):
    pieces, _, width = mine_ref.shape
    size = t_ref.shape[1]
    core, shift, base = meta_ref[0], meta_ref[2], meta_ref[3]
    group = meta_ref[4]

    def product(k, carry):
        for ref, far in ((mine_ref, 0), (other_ref, 1)):
            value = jnp.concatenate(
                [ref[k, :, j * size : (j + 1) * size] for j in range(width // size)], axis=0
            )
            n = CORES * k + (core if far == 0 else 1 - core)
            at = block_at(cols_ref[n * group + shift] - base, size)
            t_ref[CORES * k + far] = contract_last(u_ref[:, at], value)
        return carry

    lax.fori_loop(0, pieces, product, 0, unroll=4)
    o_ref[...] = jnp.zeros_like(o_ref)

    def place(k, carry):
        for far in range(CORES):
            n = CORES * k + (core if far == 0 else 1 - core)
            at = block_at(rows_ref[n * group + shift] - base, size)
            o_ref[:, at] += t_ref[CORES * k + far]
        return carry

    lax.fori_loop(0, pieces, place, 0, unroll=2)


def sparse_product(meta, rows, cols, u, mine, other, size):
    tokens, width = u.shape
    pieces, total, rank = mine.shape
    sub = size * size // rank
    values = pl.BlockSpec((pieces, sub, rank), lambda i: (0, (total - sub) // sub, 0))
    return pl.pallas_call(
        sparse_kernel,
        grid=(1,),
        in_specs=[SCALARS, SCALARS, SCALARS, whole((tokens, width)), values, values],
        out_specs=whole((tokens, width)),
        out_shape=pltpu.HBM((tokens, width), F32),
        scratch_shapes=[pltpu.VMEM((CORES * pieces, tokens, size), F32)],
        cost_estimate=cost(2 * tokens * width * rank, 2 * width * rank),
        compiler_params=LIMIT,
        name="sparse_product",
    )(meta, rows, cols, u, mine, other)


def input_kernel(meta_ref, p_ref, mine_ref, other_ref, s_ref, o_ref, ra_ref, joined_ref):
    @pl.when(pl.program_id(0) == 0)
    def _():
        total = p_ref[0].astype(F32)
        for i in range(1, p_ref.shape[0]):
            total += p_ref[i].astype(F32)
        ra_ref[...] = total.astype(BF)

    weight = both_cores(meta_ref[0], mine_ref, other_ref, joined_ref)
    o_ref[...] = (contract_last(ra_ref[...], weight) + s_ref[...]).astype(BF)


def input_grad(meta, arrived, mine, other, sparse, size):
    copies, tokens, rank = arrived.shape
    pieces, total, _ = mine.shape
    rows = total - size * size // rank
    step = pieces // GRID
    width = CORES * pieces * rows
    shard = pl.BlockSpec((step, rows, rank), lambda i: (i, 0, 0))
    slab = pl.BlockSpec((tokens, width // GRID), lambda i: (0, i))
    return pl.pallas_call(
        input_kernel,
        grid=(GRID,),
        in_specs=[SCALARS, whole((copies, tokens, rank)), shard, shard, slab],
        out_specs=slab,
        out_shape=jax.ShapeDtypeStruct((tokens, width), BF),
        scratch_shapes=[
            pltpu.VMEM((tokens, rank), BF),
            pltpu.VMEM((step, CORES, rows, rank), BF),
        ],
        cost_estimate=cost(2 * tokens * width * rank, 2 * width * rank),
        compiler_params=LIMIT,
        name="input_grad",
    )(meta, arrived, mine, other, sparse)


def block_kernel(meta_ref, rows_ref, cols_ref, st_ref, u0_ref, u1_ref, o_ref):
    blocks, size, _ = o_ref.shape
    bits = blocks.bit_length() - 1
    place, shift, base, group = meta_ref[1], meta_ref[2], meta_ref[3], meta_ref[4]

    def one(n, carry):
        turned = jnp.int32(0)
        for bit in range(bits):
            turned = turned | (((n >> bit) & 1) << (bits - 1 - bit))
        index = (place ^ turned) * group + shift
        row_at = block_at(rows_ref[index] - base, size)
        col_at = block_at(cols_ref[index] - base, size)
        left = jnp.concatenate([st_ref[0, :, row_at], st_ref[1, :, row_at]], axis=0)
        right = jnp.concatenate([u0_ref[:, col_at], u1_ref[:, col_at]], axis=0)
        o_ref[n] = contract_first(left, right)
        return carry

    lax.fori_loop(0, blocks, one, 0, unroll=4)


def block_products(meta, rows, cols, stash, u0, u1, blocks, size):
    batches, tokens, width = stash.shape
    vmem = pl.BlockSpec(memory_space=pltpu.VMEM)
    return pl.pallas_call(
        block_kernel,
        in_specs=[SCALARS, SCALARS, SCALARS, vmem, vmem, vmem],
        out_specs=vmem,
        out_shape=jax.ShapeDtypeStruct((blocks, size, size), F32),
        cost_estimate=cost(2 * batches * tokens * size * size * blocks, 6 * tokens * width),
        compiler_params=LIMIT,
        name="block_products",
    )(meta, rows, cols, stash, u0, u1)


class Data:
    def __init__(self):
        self.count = lax.axis_size("dp")
        self.ring = self.count // (FAR * CORES)
        self.place = lax.axis_index("dp")
        self.core = lax.rem(self.place, CORES)
        self.z = lax.rem(lax.div(self.place, CORES), self.ring)
        self.far = lax.div(self.place, CORES * self.ring)

    def at(self, far, z, core):
        return (far * self.ring + z % self.ring) * CORES + core

    def every(self):
        return [
            (f, z, c) for f in range(FAR) for z in range(self.ring) for c in range(CORES)
        ]

    def along(self, value, steps):
        perm = [(self.at(f, z, c), self.at(f, z + steps, c)) for f, z, c in self.every()]
        return lax.ppermute(value, "dp", perm)

    def swapped(self, value, distance):
        return lax.ppermute(value, "dp", [(p, p ^ distance) for p in range(self.count)])

    def gather(self, shard):
        got = self.swapped(shard, self.count // FAR)
        first = self.far == 0
        pair = jnp.stack([jnp.where(first, shard, got), jnp.where(first, got, shard)])
        rows, width = shard.shape
        full = jnp.zeros((FAR, self.ring, rows, width), BF)

        def put(full, piece, far, z):
            spot = (far, lax.rem(z, self.ring), 0, 0)
            return lax.dynamic_update_slice(
                full, piece[:, None], spot, allow_negative_indices=False
            )

        full = put(full, pair, 0, self.z)
        up = down = pair
        half = self.ring // 2
        for k in range(1, half):
            up = self.along(up, 1)
            down = self.along(down, -1)
            full = put(full, up, 0, self.z - k + self.ring)
            full = put(full, down, 0, self.z + k)
        up = self.along(up[:1], 1)
        down = self.along(down[1:], -1)
        full = put(full, up, 0, self.z + half)
        full = put(full, down, 1, self.z + half)
        mine = full.reshape(-1, rows, width)
        other = self.swapped(mine, 1)
        return mine, other

    def sum_at_owner(self, blocks):
        distance = 1
        while distance < self.count:
            half = blocks.shape[0] // 2
            sent = blocks[half:].astype(BF)
            blocks = blocks[:half] + self.swapped(sent, distance).astype(F32)
            distance *= 2
        return blocks


def pass_back(value):
    sections = lax.axis_size("section")
    return lax.ppermute(value, "section", [(i, i - 1) for i in range(1, sections)])


def pick(choices, which):
    out = choices[-1]
    for i in range(len(choices) - 1):
        out = jnp.where(which == i, choices[i], out)
    return out


def whole_step(cotangent, stash, factor_a, factor_b, block_vals, block_rows, block_cols):
    sections = lax.axis_size("section")
    section_pos = lax.axis_index("section")
    tensor_pos = lax.axis_index("tensor")
    tensor_count = lax.axis_size("tensor")
    data = Data()
    size = block_vals.shape[-1]
    rank = factor_b.shape[-1]
    batches = stash.shape[1]
    local_blocks = stash.shape[3] // size

    sub = size * size // rank
    lanes = rank // size
    packed = block_vals[0, 0].reshape(lanes, sub, size).transpose(1, 0, 2).reshape(sub, rank)
    a_mine, a_other = data.gather(factor_a[0])
    bv_mine, bv_other = data.gather(jnp.concatenate([factor_b[0], packed], axis=0))
    meta = jnp.stack(
        [data.core, data.place, tensor_pos, tensor_pos * local_blocks, jnp.int32(tensor_count)]
    )
    rows, cols = block_rows[0], block_cols[0]

    ups = [[cotangent[m]] for m in range(batches)]
    grads = [[] for _ in range(batches)]
    for stage in range(sections):
        for m in range(batches):
            u = ups[m][stage]
            partial = rank_partial(meta, u, a_mine, a_other, tensor_count)
            arrived = lax.all_to_all(partial, "tensor", 0, 0, tiled=True)
            sparse = sparse_product(meta, rows, cols, u, bv_mine, bv_other, size)
            grad = input_grad(meta, arrived, bv_mine, bv_other, sparse, size)
            grads[m].append(grad)
            if stage + 1 < sections:
                ups[m].append(pass_back(grad))

    turn = sections - 1 - section_pos
    used = [pick(ups[m], turn) for m in range(batches)]
    blocks = block_products(
        meta, rows, cols, stash[0], used[0], used[1], data.count, size
    )
    block_grad = data.sum_at_owner(blocks)
    grads_in = jnp.stack([pick(grads[m], turn) for m in range(batches)])
    return grads_in[None], block_grad[None]


def solution(mesh):
    in_specs = (
        P(None, "dp", "tensor"),
        P("section", None, "dp", "tensor"),
        P("section", "dp", "tensor"),
        P("section", ("tensor", "dp"), None),
        P("section", ("dp", "tensor"), None, None),
        P("section", None),
        P("section", None),
    )
    out_specs = (P("section", None, "dp", "tensor"), P("section", ("dp", "tensor"), None, None))
    return jax.shard_map(
        whole_step, mesh=mesh, in_specs=in_specs, out_specs=out_specs, check_vma=False
    )
```

```python
import jax
import jax.numpy as jnp
from jax import lax
from jax.experimental import pallas as pl
from jax.experimental.pallas import tpu as pltpu
from jax.sharding import PartitionSpec as P

BF = jnp.bfloat16
F32 = jnp.float32
FAR = 2
CORES = 2


def granted(mib):
    return pltpu.CompilerParams(vmem_limit_bytes=mib * 1024 * 1024)


LIMIT = granted(20)


def contract_last(a, b):
    return lax.dot_general(a, b, (((1,), (1,)), ((), ())), preferred_element_type=F32)


def contract_first(a, b):
    return lax.dot_general(a, b, (((0,), (0,)), ((), ())), preferred_element_type=F32)


def block_at(pos, size):
    return pl.ds(pl.multiple_of(pos * size, size), size)


SCALARS = pl.BlockSpec(memory_space=pltpu.SMEM)


def cost(flops, size):
    return pl.CostEstimate(flops=flops, bytes_accessed=size, transcendentals=0)


VMEM = pl.BlockSpec(memory_space=pltpu.VMEM)
HBM = pl.BlockSpec(memory_space=pltpu.HBM)


def join_kernel(meta_ref, mine_ref, other_ref, *outs):
    core = meta_ref[0]
    at = 0
    for out in outs:
        rows = out.shape[2]
        out[:, core] = mine_ref[:, at : at + rows]
        out[:, 1 - core] = other_ref[:, at : at + rows]
        at += rows


def joined(meta, mine, other, parts):
    pieces, _, width = mine.shape
    out = pl.pallas_call(
        join_kernel,
        in_specs=[SCALARS, VMEM, VMEM],
        out_specs=[VMEM] * len(parts),
        out_shape=[pltpu.HBM((pieces, CORES, rows, width), BF) for rows in parts],
        cost_estimate=cost(0, 2 * mine.size * CORES * 2),
        compiler_params=LIMIT,
        name="joined",
    )(meta, mine, other)
    return [x.reshape(pieces * CORES, x.shape[2], width) for x in out]


def fetched(source, target, sems, first=0):
    count = target.shape[0]
    copies = [
        pltpu.make_async_copy(source.at[i], target.at[i], sems.at[first + i])
        for i in range(count)
    ]
    for copy in copies:
        copy.start()
    return copies


def rank_kernel(u_ref, a_ref, o_ref, weight, result, sems, out_sems):
    chunks, copies = weight.shape[0], o_ref.shape[0]
    fetched(a_ref, weight, sems)
    part = result.shape[2]

    def store(i, j):
        at = o_ref.at[j, :, block_at(i, part)]
        return pltpu.make_async_copy(result.at[i], at, out_sems.at[i, j])

    def one(i, carry):
        pltpu.make_async_copy(a_ref.at[i], weight.at[i], sems.at[i]).wait()
        chunk = weight[i].reshape(part, -1)
        result[i] = contract_last(u_ref[...], chunk).astype(BF)
        for j in range(copies):
            store(i, j).start()
        return carry

    lax.fori_loop(0, chunks, one, 0)
    for i in range(chunks):
        for j in range(copies):
            store(i, j).wait()


def rank_partial(u, weight, copies):
    tokens, width = u.shape
    pieces, rows, _ = weight.shape
    rank = pieces * rows
    chunks = 4
    weight = weight.reshape(chunks, pieces // chunks, rows, width)
    return pl.pallas_call(
        rank_kernel,
        in_specs=[VMEM, HBM],
        out_specs=HBM,
        out_shape=pltpu.HBM((copies, tokens, rank), BF),
        scratch_shapes=[
            pltpu.VMEM(weight.shape, BF),
            pltpu.VMEM((chunks, tokens, rank // chunks), BF),
            pltpu.SemaphoreType.DMA((chunks,)),
            pltpu.SemaphoreType.DMA((chunks, copies)),
        ],
        cost_estimate=cost(2 * tokens * width * rank, 2 * width * rank),
        compiler_params=granted(60),
        name="rank_partial",
    )(u, weight)


def sparse_kernel(meta_ref, rows_ref, cols_ref, u_ref, v_ref, o_ref, t_ref):
    blocks, _, width = v_ref.shape
    size = t_ref.shape[1]
    shift, base, group = meta_ref[2], meta_ref[3], meta_ref[4]

    def product(n, carry):
        value = jnp.concatenate(
            [v_ref[n, :, j * size : (j + 1) * size] for j in range(width // size)], axis=0
        )
        at = block_at(cols_ref[n * group + shift] - base, size)
        t_ref[n] = contract_last(u_ref[:, at], value)
        return carry

    lax.fori_loop(0, blocks, product, 0, unroll=8)
    o_ref[...] = jnp.zeros_like(o_ref)

    def place(n, carry):
        at = block_at(rows_ref[n * group + shift] - base, size)
        o_ref[:, at] += t_ref[n]
        return carry

    lax.fori_loop(0, blocks, place, 0, unroll=4)


def sparse_product(meta, rows, cols, u, values, size):
    tokens, width = u.shape
    blocks, _, rank = values.shape
    return pl.pallas_call(
        sparse_kernel,
        in_specs=[SCALARS, SCALARS, SCALARS, VMEM, VMEM],
        out_specs=VMEM,
        out_shape=pltpu.HBM((tokens, width), F32),
        scratch_shapes=[pltpu.VMEM((blocks, tokens, size), F32)],
        cost_estimate=cost(2 * tokens * width * rank, 2 * width * rank),
        compiler_params=LIMIT,
        name="sparse_product",
    )(meta, rows, cols, u, values)


def input_kernel(p_ref, b_ref, s_ref, o_ref, parts, weight, sparse, sems, sparse_sem):
    copies, chunks = parts.shape[0], weight.shape[0]
    arrivals = fetched(p_ref, parts, sems)
    fetched(b_ref, weight, sems, copies)
    last = pltpu.make_async_copy(s_ref, sparse, sparse_sem)
    last.start()
    total = None
    for i, arrival in enumerate(arrivals):
        arrival.wait()
        part = parts[i].astype(F32)
        total = part if total is None else total + part
    act = total.astype(BF)
    last.wait()
    size = o_ref.shape[1] // chunks

    def one(i, carry):
        pltpu.make_async_copy(b_ref.at[i], weight.at[i], sems.at[copies + i]).wait()
        at = block_at(i, size)
        dense = contract_last(act, weight[i].reshape(size, -1))
        o_ref[:, at] = (dense + sparse[:, at]).astype(BF)
        return carry

    lax.fori_loop(0, chunks, one, 0)


def input_grad(arrived, weight, sparse):
    copies, tokens, rank = arrived.shape
    pieces, rows, _ = weight.shape
    chunks = 4
    weight = weight.reshape(chunks, pieces // chunks, rows, rank)
    width = pieces * rows
    return pl.pallas_call(
        input_kernel,
        in_specs=[HBM] * 3,
        out_specs=VMEM,
        out_shape=jax.ShapeDtypeStruct((tokens, width), BF),
        scratch_shapes=[
            pltpu.VMEM(arrived.shape, BF),
            pltpu.VMEM(weight.shape, BF),
            pltpu.VMEM(sparse.shape, F32),
            pltpu.SemaphoreType.DMA((copies + chunks,)),
            pltpu.SemaphoreType.DMA,
        ],
        cost_estimate=cost(2 * tokens * width * rank, 2 * width * rank),
        compiler_params=granted(63),
        name="input_grad",
    )(arrived, weight, sparse)


def block_kernel(meta_ref, rows_ref, cols_ref, st_ref, u0_ref, u1_ref, o_ref):
    blocks, size, _ = o_ref.shape
    bits = blocks.bit_length() - 1
    place, shift, base, group = meta_ref[1], meta_ref[2], meta_ref[3], meta_ref[4]

    def one(n, carry):
        turned = jnp.int32(0)
        for bit in range(bits):
            turned = turned | (((n >> bit) & 1) << (bits - 1 - bit))
        index = (place ^ turned) * group + shift
        row_at = block_at(rows_ref[index] - base, size)
        col_at = block_at(cols_ref[index] - base, size)
        left = jnp.concatenate([st_ref[0, :, row_at], st_ref[1, :, row_at]], axis=0)
        right = jnp.concatenate([u0_ref[:, col_at], u1_ref[:, col_at]], axis=0)
        o_ref[n] = contract_first(left, right)
        return carry

    lax.fori_loop(0, blocks, one, 0, unroll=4)


def block_products(meta, rows, cols, stash, u0, u1, blocks, size):
    batches, tokens, width = stash.shape
    vmem = pl.BlockSpec(memory_space=pltpu.VMEM)
    return pl.pallas_call(
        block_kernel,
        in_specs=[SCALARS, SCALARS, SCALARS, vmem, vmem, vmem],
        out_specs=vmem,
        out_shape=jax.ShapeDtypeStruct((blocks, size, size), F32),
        cost_estimate=cost(2 * batches * tokens * size * size * blocks, 6 * tokens * width),
        compiler_params=LIMIT,
        name="block_products",
    )(meta, rows, cols, stash, u0, u1)


class Data:
    def __init__(self):
        self.count = lax.axis_size("dp")
        self.ring = self.count // (FAR * CORES)
        self.place = lax.axis_index("dp")
        self.core = lax.rem(self.place, CORES)
        self.z = lax.rem(lax.div(self.place, CORES), self.ring)
        self.far = lax.div(self.place, CORES * self.ring)

    def at(self, far, z, core):
        return (far * self.ring + z % self.ring) * CORES + core

    def every(self):
        return [
            (f, z, c) for f in range(FAR) for z in range(self.ring) for c in range(CORES)
        ]

    def along(self, value, steps):
        perm = [(self.at(f, z, c), self.at(f, z + steps, c)) for f, z, c in self.every()]
        return lax.ppermute(value, "dp", perm)

    def swapped(self, value, distance):
        return lax.ppermute(value, "dp", [(p, p ^ distance) for p in range(self.count)])

    def gather(self, shard):
        got = self.swapped(shard, self.count // FAR)
        first = self.far == 0
        pair = jnp.stack([jnp.where(first, shard, got), jnp.where(first, got, shard)])
        rows, width = shard.shape
        full = jnp.zeros((FAR, self.ring, rows, width), BF)

        def put(full, piece, far, z):
            spot = (far, lax.rem(z, self.ring), 0, 0)
            return lax.dynamic_update_slice(
                full, piece[:, None], spot, allow_negative_indices=False
            )

        full = put(full, pair, 0, self.z)
        up = down = pair
        half = self.ring // 2
        for k in range(1, half):
            up = self.along(up, 1)
            down = self.along(down, -1)
            full = put(full, up, 0, self.z - k + self.ring)
            full = put(full, down, 0, self.z + k)
        up = self.along(up[:1], 1)
        down = self.along(down[1:], -1)
        full = put(full, up, 0, self.z + half)
        full = put(full, down, 1, self.z + half)
        mine = full.reshape(-1, rows, width)
        other = self.swapped(mine, 1)
        return mine, other

    def sum_at_owner(self, blocks):
        distance = 1
        while distance < self.count:
            half = blocks.shape[0] // 2
            got = self.swapped(blocks[half:].astype(BF), distance)
            blocks = blocks[:half] + got.astype(F32)
            distance *= 2
        return blocks


def pass_back(value):
    sections = lax.axis_size("section")
    return lax.ppermute(value, "section", [(i, i - 1) for i in range(1, sections)])


def pick(choices, which):
    out = choices[-1]
    for i in range(len(choices) - 1):
        out = jnp.where(which == i, choices[i], out)
    return out


def whole_step(cotangent, stash, factor_a, factor_b, block_vals, block_rows, block_cols):
    sections = lax.axis_size("section")
    section_pos = lax.axis_index("section")
    tensor_pos = lax.axis_index("tensor")
    tensor_count = lax.axis_size("tensor")
    data = Data()
    size = block_vals.shape[-1]
    rank = factor_b.shape[-1]
    batches = stash.shape[1]
    local_blocks = stash.shape[3] // size

    sub = size * size // rank
    lanes = rank // size
    packed = block_vals[0, 0].reshape(lanes, sub, size).transpose(1, 0, 2).reshape(sub, rank)
    a_mine, a_other = data.gather(factor_a[0])
    bv_mine, bv_other = data.gather(jnp.concatenate([factor_b[0], packed], axis=0))
    meta = jnp.stack(
        [data.core, data.place, tensor_pos, tensor_pos * local_blocks, jnp.int32(tensor_count)]
    )
    rows, cols = block_rows[0], block_cols[0]
    (a_full,) = joined(meta, a_mine, a_other, (factor_a.shape[1],))
    b_full, values = joined(meta, bv_mine, bv_other, (factor_b.shape[1], sub))

    ups = [[cotangent[m]] for m in range(batches)]
    grads = [[] for _ in range(batches)]
    for stage in range(sections):
        for m in range(batches):
            u = ups[m][stage]
            partial = rank_partial(u, a_full, tensor_count)
            arrived = lax.all_to_all(partial, "tensor", 0, 0, tiled=True)
            sparse = sparse_product(meta, rows, cols, u, values, size)
            grad = input_grad(arrived, b_full, sparse)
            grads[m].append(grad)
            if stage + 1 < sections:
                ups[m].append(pass_back(grad))

    turn = sections - 1 - section_pos
    used = [pick(ups[m], turn) for m in range(batches)]
    blocks = block_products(
        meta, rows, cols, stash[0], used[0], used[1], data.count, size
    )
    block_grad = data.sum_at_owner(blocks)
    grads_in = jnp.stack([pick(grads[m], turn) for m in range(batches)])
    return grads_in[None], block_grad[None]


def solution(mesh):
    in_specs = (
        P(None, "dp", "tensor"),
        P("section", None, "dp", "tensor"),
        P("section", "dp", "tensor"),
        P("section", ("tensor", "dp"), None),
        P("section", ("dp", "tensor"), None, None),
        P("section", None),
        P("section", None),
    )
    out_specs = (P("section", None, "dp", "tensor"), P("section", ("dp", "tensor"), None, None))
    return jax.shard_map(
        whole_step, mesh=mesh, in_specs=in_specs, out_specs=out_specs, check_vma=False
    )
```

```python
import functools

import jax
import jax.numpy as jnp
from jax import lax
from jax.experimental import pallas as pl
from jax.experimental.pallas import tpu as pltpu
from jax.sharding import PartitionSpec as P

BF = jnp.bfloat16
F32 = jnp.float32
FAR = 2
CORES = 2


def granted(mib):
    return pltpu.CompilerParams(vmem_limit_bytes=int(mib * 1024 * 1024))


def times(a, b):
    return jnp.dot(a, b, preferred_element_type=F32)


def block_at(pos, size):
    return pl.ds(pl.multiple_of(pos * size, size), size)


SCALARS = pl.BlockSpec(memory_space=pltpu.SMEM)


def cost(flops, size):
    return pl.CostEstimate(flops=flops, bytes_accessed=size, transcendentals=0)


VMEM = pl.BlockSpec(memory_space=pltpu.VMEM)
HBM = pl.BlockSpec(memory_space=pltpu.HBM)


def shard_copies(core, mine_ref, other_ref, joined, sems, rows):
    chunks, step = joined.shape[0], joined.shape[1]
    sides = ((mine_ref, core), (other_ref, 1 - core))

    def copy(i, side):
        ref, at = sides[side]
        return pltpu.make_async_copy(
            ref.at[pl.ds(i * step, step), rows], joined.at[i, :, at], sems.at[i, side]
        )

    for i in range(chunks):
        for side in range(CORES):
            copy(i, side).start()

    def wait(i):
        for side in range(CORES):
            copy(i, side).wait()

    return wait


def rank_kernel(meta_ref, u_ref, mine_ref, other_ref, o_ref, u, joined, result, *sems):
    u_sem, sems, out_sems = sems
    whole = pltpu.make_async_copy(u_ref, u, u_sem)
    whole.start()
    rows = pl.ds(0, joined.shape[3])
    wait = shard_copies(meta_ref[0], mine_ref, other_ref, joined, sems, rows)
    chunks, part, _ = result.shape
    copies = o_ref.shape[0]

    def store(i, j):
        return pltpu.make_async_copy(
            result.at[i], o_ref.at[j, pl.ds(i * part, part)], out_sems.at[i, j]
        )

    whole.wait()

    def one(i, carry):
        wait(i)
        result[i] = times(joined[i].reshape(part, -1), u[...]).astype(BF)
        for j in range(copies):
            store(i, j).start()
        return carry

    lax.fori_loop(0, chunks, one, 0)
    for i in range(chunks):
        for j in range(copies):
            store(i, j).wait()


def rank_partial(meta, u, mine, other, copies):
    width, tokens = u.shape
    pieces, rows, _ = mine.shape
    rank = CORES * pieces * rows
    chunks = 2
    return pl.pallas_call(
        rank_kernel,
        in_specs=[SCALARS, HBM, HBM, HBM],
        out_specs=HBM,
        out_shape=pltpu.HBM((copies, rank, tokens), BF),
        scratch_shapes=[
            pltpu.VMEM(u.shape, BF),
            pltpu.VMEM((chunks, pieces // chunks, CORES, rows, width), BF),
            pltpu.VMEM((chunks, rank // chunks, tokens), BF),
            pltpu.SemaphoreType.DMA,
            pltpu.SemaphoreType.DMA((chunks, CORES)),
            pltpu.SemaphoreType.DMA((chunks, copies)),
        ],
        cost_estimate=cost(2 * tokens * width * rank, 2 * width * rank),
        compiler_params=granted(63),
        name="rank_partial",
    )(meta, u, mine, other)


def sparse_kernel(meta_ref, rows_ref, cols_ref, u_ref, mine_ref, other_ref, o_ref, *scratch):
    u, joined, terms, total, u_sem, sems, out_sem = scratch
    blocks, size, _ = terms.shape
    _, _, _, sub, width = joined.shape
    whole = pltpu.make_async_copy(u_ref, u, u_sem)
    whole.start()
    rows = pl.ds(mine_ref.shape[1] - sub, sub)
    wait = shard_copies(meta_ref[0], mine_ref, other_ref, joined, sems, rows)
    shift, base, group = meta_ref[2], meta_ref[3], meta_ref[4]
    total[...] = jnp.zeros_like(total)
    whole.wait()
    wait(0)

    def product(n, carry):
        value = jnp.concatenate(
            [
                joined[0, n >> 1, n & 1, :, j * size : (j + 1) * size]
                for j in range(width // size)
            ],
            axis=0,
        )
        at = block_at(cols_ref[n * group + shift] - base, size)
        terms[n] = times(value, u[at, :])
        return carry

    lax.fori_loop(0, blocks, product, 0, unroll=4)

    def place(n, carry):
        at = block_at(rows_ref[n * group + shift] - base, size)
        total[at, :] += terms[n]
        return carry

    lax.fori_loop(0, blocks, place, 0, unroll=4)
    back = pltpu.make_async_copy(total, o_ref, out_sem)
    back.start()
    back.wait()


def sparse_product(meta, rows, cols, u, mine, other, size):
    width, tokens = u.shape
    pieces, _, rank = mine.shape
    sub = size * size // rank
    return pl.pallas_call(
        sparse_kernel,
        in_specs=[SCALARS, SCALARS, SCALARS, HBM, HBM, HBM],
        out_specs=HBM,
        out_shape=pltpu.HBM((width, tokens), F32),
        scratch_shapes=[
            pltpu.VMEM(u.shape, BF),
            pltpu.VMEM((1, pieces, CORES, sub, rank), BF),
            pltpu.VMEM((CORES * pieces, size, tokens), F32),
            pltpu.VMEM((width, tokens), F32),
            pltpu.SemaphoreType.DMA,
            pltpu.SemaphoreType.DMA((1, CORES)),
            pltpu.SemaphoreType.DMA,
        ],
        cost_estimate=cost(2 * tokens * width * rank, 2 * width * rank),
        compiler_params=granted(63),
        name="sparse_product",
    )(meta, rows, cols, u, mine, other)


def input_kernel(meta_ref, p_ref, mine_ref, other_ref, s_ref, o_ref, *scratch):
    parts, joined, sparse, result, part_sems, sems, sparse_sem, out_sems = scratch
    copies = parts.shape[0]
    arrivals = [
        pltpu.make_async_copy(p_ref.at[i], parts.at[i], part_sems.at[i]) for i in range(copies)
    ]
    for arrival in arrivals:
        arrival.start()
    rows = pl.ds(0, joined.shape[3])
    wait = shard_copies(meta_ref[0], mine_ref, other_ref, joined, sems, rows)
    last = pltpu.make_async_copy(s_ref, sparse, sparse_sem)
    last.start()
    total = None
    for i, arrival in enumerate(arrivals):
        arrival.wait()
        part = parts[i].astype(F32)
        total = part if total is None else total + part
    act = total.astype(BF)
    chunks, size, _ = result.shape

    def store(i):
        return pltpu.make_async_copy(
            result.at[i], o_ref.at[pl.ds(i * size, size)], out_sems.at[i]
        )

    last.wait()

    def one(i, carry):
        wait(i)
        dense = times(joined[i].reshape(size, -1), act)
        result[i] = (dense + sparse[block_at(i, size), :]).astype(BF)
        store(i).start()
        return carry

    lax.fori_loop(0, chunks, one, 0)
    for i in range(chunks):
        store(i).wait()


def input_grad(meta, arrived, mine, other, sparse, size):
    copies, rank, tokens = arrived.shape
    pieces, total, _ = mine.shape
    rows = total - size * size // rank
    chunks = 4
    width = CORES * pieces * rows
    return pl.pallas_call(
        input_kernel,
        in_specs=[SCALARS, HBM, HBM, HBM, HBM],
        out_specs=HBM,
        out_shape=pltpu.HBM((width, tokens), BF),
        scratch_shapes=[
            pltpu.VMEM(arrived.shape, BF),
            pltpu.VMEM((chunks, pieces // chunks, CORES, rows, rank), BF),
            pltpu.VMEM(sparse.shape, F32),
            pltpu.VMEM((chunks, width // chunks, tokens), BF),
            pltpu.SemaphoreType.DMA((copies,)),
            pltpu.SemaphoreType.DMA((chunks, CORES)),
            pltpu.SemaphoreType.DMA,
            pltpu.SemaphoreType.DMA((chunks,)),
        ],
        cost_estimate=cost(2 * tokens * width * rank, 2 * width * rank),
        compiler_params=granted(63),
        name="input_grad",
    )(meta, arrived, mine, other, sparse)


def block_kernel(meta_ref, rows_ref, cols_ref, st_ref, u0_ref, u1_ref, o_ref):
    blocks, size, _ = o_ref.shape
    bits = blocks.bit_length() - 1
    place, shift, base, group = meta_ref[1], meta_ref[2], meta_ref[3], meta_ref[4]

    def one(n, carry):
        turned = jnp.int32(0)
        for bit in range(bits):
            turned = turned | (((n >> bit) & 1) << (bits - 1 - bit))
        index = (place ^ turned) * group + shift
        row_at = block_at(rows_ref[index] - base, size)
        col_at = block_at(cols_ref[index] - base, size)
        left = jnp.concatenate([u0_ref[col_at, :], u1_ref[col_at, :]], axis=1)
        right = jnp.concatenate([st_ref[0, :, row_at], st_ref[1, :, row_at]], axis=0)
        o_ref[n] = times(left, right)
        return carry

    lax.fori_loop(0, blocks, one, 0, unroll=4)


def block_products(meta, rows, cols, stash, u0, u1, blocks, size):
    batches, tokens, width = stash.shape
    return pl.pallas_call(
        block_kernel,
        in_specs=[SCALARS, SCALARS, SCALARS, VMEM, VMEM, VMEM],
        out_specs=VMEM,
        out_shape=jax.ShapeDtypeStruct((blocks, size, size), F32),
        cost_estimate=cost(2 * batches * tokens * size * size * blocks, 6 * tokens * width),
        compiler_params=granted(20),
        name="block_products",
    )(meta, rows, cols, stash, u0, u1)


def finish_kernel(slot, choices, meta_ref, *refs):
    sources, o_ref, chosen, turned, sem, out_sem = refs[:choices], *refs[-5:]
    for k, source in enumerate(sources):

        @pl.when(meta_ref[5] == k)
        def _():
            copy = pltpu.make_async_copy(source, chosen, sem)
            copy.start()
            copy.wait()

    turned[...] = chosen[...].T
    out = pltpu.make_async_copy(turned, o_ref.at[slot], out_sem)
    out.start()
    out.wait()


def finished(meta, grads, slot, slots, before):
    width, tokens = grads[0].shape
    earlier = [] if before is None else [before]
    return pl.pallas_call(
        functools.partial(finish_kernel, slot, len(grads)),
        in_specs=[SCALARS] + [HBM] * (len(grads) + len(earlier)),
        out_specs=HBM,
        out_shape=pltpu.HBM((slots, tokens, width), BF),
        scratch_shapes=[
            pltpu.VMEM((width, tokens), BF),
            pltpu.VMEM((tokens, width), BF),
            pltpu.SemaphoreType.DMA,
            pltpu.SemaphoreType.DMA,
        ],
        input_output_aliases={1 + len(grads): 0} if earlier else {},
        cost_estimate=cost(0, 4 * width * tokens),
        compiler_params=granted(63),
        name="finished",
    )(meta, *grads, *earlier)


class Data:
    def __init__(self):
        self.count = lax.axis_size("dp")
        self.ring = self.count // (FAR * CORES)
        self.place = lax.axis_index("dp")
        self.core = lax.rem(self.place, CORES)
        self.z = lax.rem(lax.div(self.place, CORES), self.ring)
        self.far = lax.div(self.place, CORES * self.ring)

    def at(self, far, z, core):
        return (far * self.ring + z % self.ring) * CORES + core

    def every(self):
        return [
            (f, z, c) for f in range(FAR) for z in range(self.ring) for c in range(CORES)
        ]

    def along(self, value, steps):
        perm = [(self.at(f, z, c), self.at(f, z + steps, c)) for f, z, c in self.every()]
        return lax.ppermute(value, "dp", perm)

    def swapped(self, value, distance):
        return lax.ppermute(value, "dp", [(p, p ^ distance) for p in range(self.count)])

    def gather(self, shard):
        got = self.swapped(shard, self.count // FAR)
        first = self.far == 0
        pair = jnp.stack([jnp.where(first, shard, got), jnp.where(first, got, shard)])
        rows, width = shard.shape
        full = jnp.zeros((FAR, self.ring, rows, width), BF)

        def put(full, piece, far, z):
            spot = (far, lax.rem(z, self.ring), 0, 0)
            return lax.dynamic_update_slice(
                full, piece[:, None], spot, allow_negative_indices=False
            )

        full = put(full, pair, 0, self.z)
        up = down = pair
        half = self.ring // 2
        for k in range(1, half):
            up = self.along(up, 1)
            down = self.along(down, -1)
            full = put(full, up, 0, self.z - k + self.ring)
            full = put(full, down, 0, self.z + k)
        up = self.along(up[:1], 1)
        down = self.along(down[1:], -1)
        full = put(full, up, 0, self.z + half)
        full = put(full, down, 1, self.z + half)
        mine = full.reshape(-1, rows, width)
        other = self.swapped(mine, 1)
        return mine, other

    def sum_at_owner(self, blocks):
        distance = 1
        while distance < self.count:
            half = blocks.shape[0] // 2
            got = self.swapped(blocks[half:].astype(BF), distance)
            blocks = blocks[:half] + got.astype(F32)
            distance *= 2
        return blocks


def pass_back(value):
    sections = lax.axis_size("section")
    return lax.ppermute(value, "section", [(i, i - 1) for i in range(1, sections)])


def pick(choices, which):
    out = choices[-1]
    for i in range(len(choices) - 1):
        out = jnp.where(which == i, choices[i], out)
    return out


def whole_step(cotangent, stash, factor_a, factor_b, block_vals, block_rows, block_cols):
    sections = lax.axis_size("section")
    section_pos = lax.axis_index("section")
    tensor_pos = lax.axis_index("tensor")
    tensor_count = lax.axis_size("tensor")
    data = Data()
    size = block_vals.shape[-1]
    rank = factor_b.shape[-1]
    batches = stash.shape[1]
    local_blocks = stash.shape[3] // size

    sub = size * size // rank
    lanes = rank // size
    packed = block_vals[0, 0].reshape(lanes, sub, size).transpose(1, 0, 2).reshape(sub, rank)
    a_mine, a_other = data.gather(factor_a[0])
    bv_mine, bv_other = data.gather(jnp.concatenate([factor_b[0], packed], axis=0))
    turn = sections - 1 - section_pos
    meta = jnp.stack(
        [
            data.core,
            data.place,
            tensor_pos,
            tensor_pos * local_blocks,
            jnp.int32(tensor_count),
            turn,
        ]
    )
    rows, cols = block_rows[0], block_cols[0]

    ups = [[cotangent[m].T] for m in range(batches)]
    grads = [[] for _ in range(batches)]
    for stage in range(sections):
        for m in range(batches):
            u = ups[m][stage]
            partial = rank_partial(meta, u, a_mine, a_other, tensor_count)
            arrived = lax.all_to_all(partial, "tensor", 0, 0, tiled=True)
            sparse = sparse_product(meta, rows, cols, u, bv_mine, bv_other, size)
            grad = input_grad(meta, arrived, bv_mine, bv_other, sparse, size)
            grads[m].append(grad)
            if stage + 1 < sections:
                ups[m].append(pass_back(grad))

    used = [pick(ups[m], turn) for m in range(batches)]
    blocks = block_products(
        meta, rows, cols, stash[0], used[0], used[1], data.count, size
    )
    block_grad = data.sum_at_owner(blocks).swapaxes(1, 2)
    grads_in = None
    for m in range(batches):
        grads_in = finished(meta, grads[m], m, batches, grads_in)
    return grads_in[None], block_grad[None]


def solution(mesh):
    in_specs = (
        P(None, "dp", "tensor"),
        P("section", None, "dp", "tensor"),
        P("section", "dp", "tensor"),
        P("section", ("tensor", "dp"), None),
        P("section", ("dp", "tensor"), None, None),
        P("section", None),
        P("section", None),
    )
    out_specs = (P("section", None, "dp", "tensor"), P("section", ("dp", "tensor"), None, None))
    return jax.shard_map(
        whole_step, mesh=mesh, in_specs=in_specs, out_specs=out_specs, check_vma=False
    )
```

```python
import functools

import jax
import jax.numpy as jnp
from jax import lax
from jax.experimental import pallas as pl
from jax.experimental.pallas import tpu as pltpu
from jax.sharding import PartitionSpec as P

BF = jnp.bfloat16
F32 = jnp.float32
FAR = 2
CORES = 2


def granted(mib):
    return pltpu.CompilerParams(vmem_limit_bytes=int(mib * 1024 * 1024))


def times(a, b):
    return jnp.dot(a, b, preferred_element_type=F32)


def block_at(pos, size):
    return pl.ds(pl.multiple_of(pos * size, size), size)


HELD = 40
SCALARS = pl.BlockSpec(memory_space=pltpu.SMEM)


def cost(flops, size):
    return pl.CostEstimate(flops=flops, bytes_accessed=size, transcendentals=0)


VMEM = pl.BlockSpec(memory_space=pltpu.VMEM)
HBM = pl.BlockSpec(memory_space=pltpu.HBM)


def shard_copies(core, mine_ref, other_ref, joined, sems, rows):
    chunks, step = joined.shape[0], joined.shape[1]
    sides = ((mine_ref, core), (other_ref, 1 - core))

    def copy(i, side):
        ref, at = sides[side]
        return pltpu.make_async_copy(
            ref.at[pl.ds(i * step, step), rows], joined.at[i, :, at], sems.at[i, side]
        )

    for i in range(chunks):
        for side in range(CORES):
            copy(i, side).start()

    def wait(i):
        for side in range(CORES):
            copy(i, side).wait()

    return wait


def rank_kernel(meta_ref, u_ref, mine_ref, other_ref, o_ref, u, joined, result, *sems):
    u_sem, sems, out_sems = sems
    whole = pltpu.make_async_copy(u_ref, u, u_sem)
    whole.start()
    rows = pl.ds(0, joined.shape[3])
    wait = shard_copies(meta_ref[0], mine_ref, other_ref, joined, sems, rows)
    chunks, part, _ = result.shape
    copies = o_ref.shape[0]

    def store(i, j):
        return pltpu.make_async_copy(
            result.at[i], o_ref.at[j, pl.ds(i * part, part)], out_sems.at[i, j]
        )

    whole.wait()

    def one(i, carry):
        wait(i)
        result[i] = times(joined[i].reshape(part, -1), u[...]).astype(BF)
        for j in range(copies):
            store(i, j).start()
        return carry

    lax.fori_loop(0, chunks, one, 0)
    for i in range(chunks):
        for j in range(copies):
            store(i, j).wait()


def rank_partial(meta, u, mine, other, copies):
    width, tokens = u.shape
    pieces, rows, _ = mine.shape
    rank = CORES * pieces * rows
    chunks = 2
    return pl.pallas_call(
        rank_kernel,
        in_specs=[SCALARS, HBM, HBM, HBM],
        out_specs=HBM,
        out_shape=pltpu.HBM((copies, rank, tokens), BF),
        scratch_shapes=[
            pltpu.VMEM(u.shape, BF),
            pltpu.VMEM((chunks, pieces // chunks, CORES, rows, width), BF),
            pltpu.VMEM((chunks, rank // chunks, tokens), BF),
            pltpu.SemaphoreType.DMA,
            pltpu.SemaphoreType.DMA((chunks, CORES)),
            pltpu.SemaphoreType.DMA((chunks, copies)),
        ],
        cost_estimate=cost(2 * tokens * width * rank, 2 * width * rank),
        compiler_params=granted(63),
        name="rank_partial",
    )(meta, u, mine, other)


def held_kernel(u_ref, a_ref, o_ref, u, result, u_sem, out_sems):
    whole = pltpu.make_async_copy(u_ref, u, u_sem)
    whole.start()
    chunks, part, _ = result.shape
    copies = o_ref.shape[0]
    step = a_ref.shape[0] // chunks

    def store(i, j):
        return pltpu.make_async_copy(
            result.at[i], o_ref.at[j, pl.ds(i * part, part)], out_sems.at[i, j]
        )

    whole.wait()
    for i in range(chunks):
        weight = a_ref[i * step : (i + 1) * step].reshape(part, -1)
        result[i] = times(weight, u[...]).astype(BF)
        for j in range(copies):
            store(i, j).start()
    for i in range(chunks):
        for j in range(copies):
            store(i, j).wait()


def rank_held(u, weight, copies):
    width, tokens = u.shape
    pieces, cores, rows, _ = weight.shape
    rank = pieces * cores * rows
    chunks = 2
    return pl.pallas_call(
        held_kernel,
        in_specs=[HBM, VMEM],
        out_specs=HBM,
        out_shape=pltpu.HBM((copies, rank, tokens), BF),
        scratch_shapes=[
            pltpu.VMEM(u.shape, BF),
            pltpu.VMEM((chunks, rank // chunks, tokens), BF),
            pltpu.SemaphoreType.DMA,
            pltpu.SemaphoreType.DMA((chunks, copies)),
        ],
        cost_estimate=cost(2 * tokens * width * rank, 2 * width * rank),
        compiler_params=granted(HELD),
        name="rank_held",
    )(u, weight)


def sparse_kernel(
    hold, meta_ref, rows_ref, cols_ref, u_ref, mine_ref, other_ref, a_mine, a_other, o_ref, *rest
):
    u, joined, terms, total, u_sem, sems, out_sem, held_sems = rest[-8:]
    blocks, size, _ = terms.shape
    _, _, _, sub, width = joined.shape
    whole = pltpu.make_async_copy(u_ref, u, u_sem)
    whole.start()
    rows = pl.ds(mine_ref.shape[1] - sub, sub)
    wait = shard_copies(meta_ref[0], mine_ref, other_ref, joined, sems, rows)
    shift, base, group = meta_ref[2], meta_ref[3], meta_ref[4]
    if hold:
        core = meta_ref[0]
        held = [
            pltpu.make_async_copy(ref, rest[0].at[:, at], held_sems.at[side])
            for side, (ref, at) in enumerate(((a_mine, core), (a_other, 1 - core)))
        ]
        for copy in held:
            copy.start()
    total[...] = jnp.zeros_like(total)
    whole.wait()
    wait(0)

    def product(n, carry):
        value = jnp.concatenate(
            [
                joined[0, n >> 1, n & 1, :, j * size : (j + 1) * size]
                for j in range(width // size)
            ],
            axis=0,
        )
        at = block_at(cols_ref[n * group + shift] - base, size)
        terms[n] = times(value, u[at, :])
        return carry

    lax.fori_loop(0, blocks, product, 0, unroll=4)

    def place(n, carry):
        at = block_at(rows_ref[n * group + shift] - base, size)
        total[at, :] += terms[n]
        return carry

    lax.fori_loop(0, blocks, place, 0, unroll=4)
    back = pltpu.make_async_copy(total, o_ref, out_sem)
    back.start()
    back.wait()
    if hold:
        for copy in held:
            copy.wait()


def sparse_product(meta, rows, cols, u, mine, other, a_mine, a_other, size, hold):
    width, tokens = u.shape
    a_pieces, a_rows, _ = a_mine.shape
    pieces, _, rank = mine.shape
    sub = size * size // rank
    held = [pltpu.VMEM((a_pieces, CORES, a_rows, width), BF)] if hold else []
    out = pl.pallas_call(
        functools.partial(sparse_kernel, hold),
        in_specs=[SCALARS, SCALARS, SCALARS, HBM, HBM, HBM, HBM, HBM],
        out_specs=[HBM] + [VMEM] * len(held),
        out_shape=[pltpu.HBM((width, tokens), F32)] + held,
        scratch_shapes=[
            pltpu.VMEM(u.shape, BF),
            pltpu.VMEM((1, pieces, CORES, sub, rank), BF),
            pltpu.VMEM((CORES * pieces, size, tokens), F32),
            pltpu.VMEM((width, tokens), F32),
            pltpu.SemaphoreType.DMA,
            pltpu.SemaphoreType.DMA((1, CORES)),
            pltpu.SemaphoreType.DMA,
            pltpu.SemaphoreType.DMA((CORES,)),
        ],
        cost_estimate=cost(2 * tokens * width * rank, 2 * width * rank),
        compiler_params=granted(HELD),
        name="sparse_product",
    )(meta, rows, cols, u, mine, other, a_mine, a_other)
    return out if hold else (out[0], None)


def input_kernel(meta_ref, p_ref, mine_ref, other_ref, s_ref, o_ref, *scratch):
    parts, joined, sparse, result, part_sems, sems, sparse_sem, out_sems = scratch
    copies = parts.shape[0]
    arrivals = [
        pltpu.make_async_copy(p_ref.at[i], parts.at[i], part_sems.at[i]) for i in range(copies)
    ]
    for arrival in arrivals:
        arrival.start()
    last = pltpu.make_async_copy(s_ref, sparse, sparse_sem)
    last.start()
    rows = pl.ds(0, joined.shape[3])
    wait = shard_copies(meta_ref[0], mine_ref, other_ref, joined, sems, rows)
    total = None
    for i, arrival in enumerate(arrivals):
        arrival.wait()
        part = parts[i].astype(F32)
        total = part if total is None else total + part
    act = total.astype(BF)
    chunks, size, _ = result.shape

    def store(i):
        return pltpu.make_async_copy(
            result.at[i], o_ref.at[pl.ds(i * size, size)], out_sems.at[i]
        )

    last.wait()

    def one(i, carry):
        wait(i)
        dense = times(joined[i].reshape(size, -1), act)
        result[i] = (dense + sparse[block_at(i, size), :]).astype(BF)
        store(i).start()
        return carry

    lax.fori_loop(0, chunks, one, 0)
    for i in range(chunks):
        store(i).wait()


def input_grad(meta, arrived, mine, other, sparse, size):
    copies, rank, tokens = arrived.shape
    pieces, total, _ = mine.shape
    rows = total - size * size // rank
    chunks = 4
    width = CORES * pieces * rows
    return pl.pallas_call(
        input_kernel,
        in_specs=[SCALARS, HBM, HBM, HBM, HBM],
        out_specs=HBM,
        out_shape=pltpu.HBM((width, tokens), BF),
        scratch_shapes=[
            pltpu.VMEM(arrived.shape, BF),
            pltpu.VMEM((chunks, pieces // chunks, CORES, rows, rank), BF),
            pltpu.VMEM(sparse.shape, F32),
            pltpu.VMEM((chunks, width // chunks, tokens), BF),
            pltpu.SemaphoreType.DMA((copies,)),
            pltpu.SemaphoreType.DMA((chunks, CORES)),
            pltpu.SemaphoreType.DMA,
            pltpu.SemaphoreType.DMA((chunks,)),
        ],
        cost_estimate=cost(2 * tokens * width * rank, 2 * width * rank),
        compiler_params=granted(63),
        name="input_grad",
    )(meta, arrived, mine, other, sparse)


def block_kernel(meta_ref, rows_ref, cols_ref, st_ref, u0_ref, u1_ref, o_ref):
    blocks, size, _ = o_ref.shape
    bits = blocks.bit_length() - 1
    place, shift, base, group = meta_ref[1], meta_ref[2], meta_ref[3], meta_ref[4]

    def one(n, carry):
        turned = jnp.int32(0)
        for bit in range(bits):
            turned = turned | (((n >> bit) & 1) << (bits - 1 - bit))
        index = (place ^ turned) * group + shift
        row_at = block_at(rows_ref[index] - base, size)
        col_at = block_at(cols_ref[index] - base, size)
        left = jnp.concatenate([u0_ref[col_at, :], u1_ref[col_at, :]], axis=1)
        right = jnp.concatenate([st_ref[0, :, row_at], st_ref[1, :, row_at]], axis=0)
        o_ref[n] = times(left, right)
        return carry

    lax.fori_loop(0, blocks, one, 0, unroll=4)


def block_products(meta, rows, cols, stash, u0, u1, blocks, size):
    batches, tokens, width = stash.shape
    return pl.pallas_call(
        block_kernel,
        in_specs=[SCALARS, SCALARS, SCALARS, VMEM, VMEM, VMEM],
        out_specs=VMEM,
        out_shape=jax.ShapeDtypeStruct((blocks, size, size), F32),
        cost_estimate=cost(2 * batches * tokens * size * size * blocks, 6 * tokens * width),
        compiler_params=granted(20),
        name="block_products",
    )(meta, rows, cols, stash, u0, u1)


def finish_kernel(slot, choices, meta_ref, *refs):
    sources, o_ref, chosen, turned, sem, out_sem = refs[:choices], *refs[-5:]
    for k, source in enumerate(sources):

        @pl.when(meta_ref[5] == k)
        def _():
            copy = pltpu.make_async_copy(source, chosen, sem)
            copy.start()
            copy.wait()

    turned[...] = chosen[...].T
    out = pltpu.make_async_copy(turned, o_ref.at[slot], out_sem)
    out.start()
    out.wait()


def finished(meta, grads, slot, slots, before):
    width, tokens = grads[0].shape
    earlier = [] if before is None else [before]
    return pl.pallas_call(
        functools.partial(finish_kernel, slot, len(grads)),
        in_specs=[SCALARS] + [HBM] * (len(grads) + len(earlier)),
        out_specs=HBM,
        out_shape=pltpu.HBM((slots, tokens, width), BF),
        scratch_shapes=[
            pltpu.VMEM((width, tokens), BF),
            pltpu.VMEM((tokens, width), BF),
            pltpu.SemaphoreType.DMA,
            pltpu.SemaphoreType.DMA,
        ],
        input_output_aliases={1 + len(grads): 0} if earlier else {},
        cost_estimate=cost(0, 4 * width * tokens),
        compiler_params=granted(63),
        name="finished",
    )(meta, *grads, *earlier)


class Data:
    def __init__(self):
        self.count = lax.axis_size("dp")
        self.ring = self.count // (FAR * CORES)
        self.place = lax.axis_index("dp")
        self.core = lax.rem(self.place, CORES)
        self.z = lax.rem(lax.div(self.place, CORES), self.ring)
        self.far = lax.div(self.place, CORES * self.ring)

    def at(self, far, z, core):
        return (far * self.ring + z % self.ring) * CORES + core

    def every(self):
        return [
            (f, z, c) for f in range(FAR) for z in range(self.ring) for c in range(CORES)
        ]

    def along(self, value, steps):
        perm = [(self.at(f, z, c), self.at(f, z + steps, c)) for f, z, c in self.every()]
        return lax.ppermute(value, "dp", perm)

    def swapped(self, value, distance):
        return lax.ppermute(value, "dp", [(p, p ^ distance) for p in range(self.count)])

    def gather(self, shard):
        got = self.swapped(shard, self.count // FAR)
        first = self.far == 0
        pair = jnp.stack([jnp.where(first, shard, got), jnp.where(first, got, shard)])
        rows, width = shard.shape
        full = jnp.zeros((FAR, self.ring, rows, width), BF)

        def put(full, piece, far, z):
            spot = (far, lax.rem(z, self.ring), 0, 0)
            return lax.dynamic_update_slice(
                full, piece[:, None], spot, allow_negative_indices=False
            )

        full = put(full, pair, 0, self.z)
        up = down = pair
        half = self.ring // 2
        for k in range(1, half):
            up = self.along(up, 1)
            down = self.along(down, -1)
            full = put(full, up, 0, self.z - k + self.ring)
            full = put(full, down, 0, self.z + k)
        up = self.along(up[:1], 1)
        down = self.along(down[1:], -1)
        full = put(full, up, 0, self.z + half)
        full = put(full, down, 1, self.z + half)
        mine = full.reshape(-1, rows, width)
        other = self.swapped(mine, 1)
        return mine, other

    def sum_at_owner(self, blocks):
        distance = 1
        while distance < self.count:
            half = blocks.shape[0] // 2
            got = self.swapped(blocks[half:].astype(BF), distance)
            blocks = blocks[:half] + got.astype(F32)
            distance *= 2
        return blocks


def pass_back(value):
    sections = lax.axis_size("section")
    return lax.ppermute(value, "section", [(i, i - 1) for i in range(1, sections)])


def pick(choices, which):
    out = choices[-1]
    for i in range(len(choices) - 1):
        out = jnp.where(which == i, choices[i], out)
    return out


def whole_step(cotangent, stash, factor_a, factor_b, block_vals, block_rows, block_cols):
    sections = lax.axis_size("section")
    section_pos = lax.axis_index("section")
    tensor_pos = lax.axis_index("tensor")
    tensor_count = lax.axis_size("tensor")
    data = Data()
    size = block_vals.shape[-1]
    rank = factor_b.shape[-1]
    batches = stash.shape[1]
    local_blocks = stash.shape[3] // size

    sub = size * size // rank
    lanes = rank // size
    packed = block_vals[0, 0].reshape(lanes, sub, size).transpose(1, 0, 2).reshape(sub, rank)
    a_mine, a_other = data.gather(factor_a[0])
    bv_mine, bv_other = data.gather(jnp.concatenate([factor_b[0], packed], axis=0))
    turn = sections - 1 - section_pos
    meta = jnp.stack(
        [
            data.core,
            data.place,
            tensor_pos,
            tensor_pos * local_blocks,
            jnp.int32(tensor_count),
            turn,
        ]
    )
    rows, cols = block_rows[0], block_cols[0]

    ups = [[cotangent[m].T] for m in range(batches)]
    grads = [[] for _ in range(batches)]
    held = None
    for stage in range(sections):
        for m in range(batches):
            u = ups[m][stage]
            if held is None or stage == 0:
                partial = rank_partial(meta, u, a_mine, a_other, tensor_count)
            else:
                partial = rank_held(u, held, tensor_count)
            arrived = lax.all_to_all(partial, "tensor", 0, 0, tiled=True)
            last = stage + 1 == sections and m + 1 == batches
            hold = not last and (stage, m) != (0, 0)
            sparse, held = sparse_product(
                meta, rows, cols, u, bv_mine, bv_other, a_mine, a_other, size, hold
            )
            grad = input_grad(meta, arrived, bv_mine, bv_other, sparse, size)
            grads[m].append(grad)
            if stage + 1 < sections:
                ups[m].append(pass_back(grad))

    used = [pick(ups[m], turn) for m in range(batches)]
    blocks = block_products(
        meta, rows, cols, stash[0], used[0], used[1], data.count, size
    )
    block_grad = data.sum_at_owner(blocks).swapaxes(1, 2)
    grads_in = None
    for m in range(batches):
        grads_in = finished(meta, grads[m], m, batches, grads_in)
    return grads_in[None], block_grad[None]


def solution(mesh):
    in_specs = (
        P(None, "dp", "tensor"),
        P("section", None, "dp", "tensor"),
        P("section", "dp", "tensor"),
        P("section", ("tensor", "dp"), None),
        P("section", ("dp", "tensor"), None, None),
        P("section", None),
        P("section", None),
    )
    out_specs = (P("section", None, "dp", "tensor"), P("section", ("dp", "tensor"), None, None))
    return jax.shard_map(
        whole_step, mesh=mesh, in_specs=in_specs, out_specs=out_specs, check_vma=False
    )
```
